32 devices in a mesh: seq: 8 (over z, y), batch: 4 (over x, core).
Axes of the slice: x: 2, y: 2, z: 4, core: 2. Of those that a mesh axis runs over, the one named last changes fastest.
Arguments:
- inputs: bfloat16 [8192, 4096], P(('batch', 'seq')), parts along dimension 0, may hold values from -6 to 6
- recur_weight: bfloat16 [16, 256, 256], replicated, may hold values from -0.375 to 0.375
- input_weight: bfloat16 [16, 256, 256], replicated, may hold values from -0.375 to 0.375
- recur_bias: float32 [4096], replicated, may hold values from -4 to 4
- input_bias: float32 [4096], replicated, may hold values from -4 to 4
- decay_rate: float32 [4096], replicated, may hold values from 4.8828124e-06 to 0.02
- kv_weight: bfloat16 [4096, 512], replicated, may hold values from -61 to 61
Outputs:
- attended: bfloat16 [8192, 4096], P(('batch', 'seq')), parts along dimension 0
The draws below stay inside these ranges and needn't reach their ends.
There are 4 independent parts, one for each index of `batch`. The reference program is written for one: setup_inputs(seed, part) draws one part's arguments, and reference() takes and returns one part's arrays. A program takes and returns all parts, laid end to end along the dimension named above; an argument that names none is the same for every part. Nothing has to cross between parts.
All inputs are finite; a program needn't handle non-finite values.
Results may differ from the reference program's by a relative error of at most 0.03.
Values may be sent and summed in bfloat16 or wider, within the bound.
A program may use at most 128 MiB of HBM per device.

```python
import math
import jax
import jax.numpy as jnp
from jax import lax

D = 4096
HEAD_DIM = 256
BLOCKS = 16
BLOCK_WIDTH = 256
WINDOW = 2048
TOK_DEV = 256
SEQ_LEN = 2048


def draw_kv_weight(key, part):
    first, second = jax.random.split(jax.random.fold_in(key, 7331))
    heads = D // HEAD_DIM
    base = jax.random.normal(first, (D, 2 * HEAD_DIM), jnp.float32) * D ** (-0.5)
    base = jnp.clip(base, -6.0 * D ** (-0.5), 6.0 * D ** (-0.5))
    level = jax.random.uniform(second, (heads,), jnp.float32)
    lowest = 2.0 / HEAD_DIM ** 0.5
    highest = 24.0 / HEAD_DIM ** 0.5
    strength = jnp.exp(jnp.log(lowest) + level * (jnp.log(highest) - jnp.log(lowest)))
    identity = jnp.eye(HEAD_DIM, dtype=jnp.float32)
    aligned = (strength[:, None, None] * identity[None, :, :]).reshape(D, HEAD_DIM)
    key_cols = base[:, :HEAD_DIM] + aligned
    return jnp.concatenate([key_cols, base[:, HEAD_DIM:]], axis=1).astype(jnp.bfloat16)


def shard_levels(rng, shape, cuts, low, top_value):
    def one(dim, blocks):
        steps = jax.random.uniform(jax.random.fold_in(jax.random.fold_in(rng, 6), dim), (blocks,), jnp.float32, low / len(cuts), top_value / len(cuts))
        return jnp.repeat(jnp.exp(steps), shape[dim] // blocks).reshape((-1,) + (1,) * (len(shape) - dim - 1))

    loudness = one(*cuts[0])
    for cut in cuts[1:]:
        loudness = loudness * one(*cut)
    return loudness


def noise(own_key, dims, deviation, limit, shards=(), kind=jnp.bfloat16):
    level = shard_levels(own_key, dims, shards, -0.22, 0.18) if shards else 1.0
    values = jax.random.normal(own_key, dims, jnp.float32) * deviation * level
    return jnp.minimum(jnp.maximum(values, -limit), limit).astype(kind)


def setup_inputs(seed: int = 0, part: int = 0) -> dict:
    streams_of = jax.random.split(jax.random.key(seed), 8)
    part_splits = jax.random.split(jax.random.fold_in(streams_of[7], part), 8)
    return {
        "inputs": noise(part_splits[0], (SEQ_LEN, D), 1.0, 6.0, ((0, 8),)),
        "recur_weight": noise(streams_of[1], (BLOCKS, BLOCK_WIDTH, BLOCK_WIDTH), BLOCK_WIDTH ** -0.5, 0.375),
        "input_weight": noise(streams_of[2], (BLOCKS, BLOCK_WIDTH, BLOCK_WIDTH), BLOCK_WIDTH ** -0.5, 0.375),
        "recur_bias": noise(streams_of[3], (D,), 1.0, 4.0, (), jnp.float32),
        "input_bias": noise(streams_of[4], (D,), 1.0, 4.0, (), jnp.float32),
        "decay_rate": jnp.clip(jnp.exp(jax.random.uniform(streams_of[5], (D,), jnp.float32, math.log(4.882812390860636e-06), math.log(0.02))), 4.882812390860636e-06, 0.02),
        "kv_weight": draw_kv_weight(jax.random.fold_in(streams_of[7], 71), part),
    }


def combine_steps(earlier, later):
    return (earlier[0] * later[0], later[0] * earlier[1] + later[1])

def block_gate(inputs, weight, bias):
    total_rows = inputs.shape[0]
    split = inputs.astype(jnp.float32).reshape(total_rows, weight.shape[0], weight.shape[1])
    mixed = jnp.einsum('tbi,bio->tbo', split, weight.astype(jnp.float32))
    return jax.nn.sigmoid(mixed.reshape(total_rows, -1) + bias)

def reference(inputs, recur_weight, input_weight, recur_bias, input_bias, decay_rate, kv_weight):
    total_rows = inputs.shape[0]
    width_all = inputs.shape[1]
    recurrence = block_gate(inputs, recur_weight, recur_bias)
    input_gate = block_gate(inputs, input_weight, input_bias)
    decay_step = jnp.exp(-8.0 * recurrence * decay_rate)
    driven = jnp.sqrt(1.0 - decay_step * decay_step) * (input_gate * inputs.astype(jnp.float32))
    cumulative, state = lax.associative_scan(combine_steps, (decay_step, driven), axis=0)
    hidden = state.astype(jnp.bfloat16)
    keyval = jnp.dot(hidden, kv_weight, preferred_element_type=jnp.float32).astype(jnp.bfloat16)
    head_dim = kv_weight.shape[1] // 2
    heads = width_all // head_dim
    reach = (WINDOW + TOK_DEV - 2) // TOK_DEV
    padded = jnp.concatenate([jnp.zeros((reach * TOK_DEV, 2 * head_dim), jnp.bfloat16), keyval], axis=0)
    scale = head_dim ** (-0.5)

    def block_out(index):
        start = (index * TOK_DEV).astype(jnp.int32)
        local_kv = lax.dynamic_slice_in_dim(padded, start, (reach + 1) * TOK_DEV, 0).astype(jnp.float32)
        queries = lax.dynamic_slice_in_dim(hidden, start, TOK_DEV, 0).astype(jnp.float32)
        queries = queries.reshape(TOK_DEV, heads, head_dim).transpose(1, 0, 2)
        keys = local_kv[:, :head_dim]
        values = local_kv[:, head_dim:]
        query_pos = start + jnp.arange(TOK_DEV, dtype=jnp.int32)
        key_pos = start - reach * TOK_DEV + jnp.arange((reach + 1) * TOK_DEV, dtype=jnp.int32)
        allowed = (key_pos[None, :] <= query_pos[:, None]) & (key_pos[None, :] > query_pos[:, None] - WINDOW) & (key_pos[None, :] >= 0)
        scores = jnp.einsum('htd,kd->htk', queries, keys) * scale
        scores = jnp.where(allowed[None], scores, -1e+30)
        highest = lax.optimization_barrier(jnp.max(scores, axis=-1, keepdims=True))
        expo = jnp.exp(scores - highest)
        weights = (expo / lax.optimization_barrier(jnp.sum(expo, axis=-1, keepdims=True))).astype(jnp.bfloat16)
        result = jnp.einsum('htk,kd->htd', weights.astype(jnp.float32), values).astype(jnp.bfloat16)
        return result.transpose(1, 0, 2).reshape(TOK_DEV, width_all)
    blocks_out = lax.map(block_out, jnp.arange(total_rows // TOK_DEV, dtype=jnp.int32))
    return blocks_out.reshape(total_rows, width_all)
```

```python
import functools
import math

import jax
import jax.numpy as jnp
from jax import lax
from jax.experimental import pallas as pl
from jax.experimental.pallas import tpu as pltpu
from jax.sharding import PartitionSpec as P

WINDOW = 2048
SUB = 8
PIECES = 2
MESH = pl.DeviceIdType.MESH
LOG2E = math.log2(math.e)
F32 = jnp.float32
BF16 = jnp.bfloat16


def dot(a, b):
    return jnp.dot(a, b, preferred_element_type=F32)


def dot_t(a, b):
    return lax.dot_general(a, b, (((1,), (1,)), ((), ())), preferred_element_type=F32)


def fused(
    n, cols, reach, scale,
    x_hbm, rw_hbm, iw_hbm, rb, ib, dr, kvw_hbm,
    out,
    xv, rwv, iwv, kvw, perm, unperm, pre_a, pre_b, cum, loc, seg_a, seg_s, sum_send, sum_recv,
    carry, hid, qn, kvb, top, low, acc, bias,
    in_sem, kvw_sem, s_send, s_recv, z_send, y_send, kv_recv,
):
    me = lax.axis_index("seq")
    row = me // cols
    col = me % cols
    blocks, tok, width = xv.shape
    seg = tok // SUB
    groups = blocks // 2
    head_dim = width
    levels = z_send.shape[0] - 1
    piece_rows = tok // PIECES

    def in_copies(b):
        at = pl.ds(pl.multiple_of(b * width, width), width)
        return (
            pltpu.make_async_copy(x_hbm.at[:, at], xv.at[b], in_sem.at[0, b]),
            pltpu.make_async_copy(rw_hbm.at[b], rwv.at[b], in_sem.at[1, b]),
            pltpu.make_async_copy(iw_hbm.at[b], iwv.at[b], in_sem.at[2, b]),
        )

    @pl.loop(0, blocks)
    def _(b):
        for copy in in_copies(b):
            copy.start()

    kvw_copy = pltpu.make_async_copy(kvw_hbm, kvw, kvw_sem)
    kvw_copy.start()

    barrier = pltpu.get_barrier_semaphore()

    @pl.loop(1, n)
    def _(d):
        pl.semaphore_signal(
            barrier, inc=1, device_id={"seq": lax.rem(me + d, n)}, device_id_type=MESH
        )

    first = lax.broadcasted_iota(jnp.int32, (tok, tok), 0)
    second = lax.broadcasted_iota(jnp.int32, (tok, tok), 1)
    place_1 = second // SUB + seg * (second % SUB)
    place_0 = first // SUB + seg * (first % SUB)
    perm[...] = jnp.where(second == place_0, 1.0, 0.0).astype(BF16)
    unperm[...] = jnp.where(first == place_1, 1.0, 0.0).astype(BF16)
    bias[...] = jnp.where(place_1 <= first, 0.0, -1e30)

    def mats(b, pre):
        for copy in in_copies(b):
            copy.wait()
        moved = dot(perm[...], xv[b])
        small = moved.astype(BF16)
        pre[0] = moved
        pre[1] = dot(small, rwv[b])
        pre[2] = dot(small, iwv[b])

    def gates(b, g, half, pre):
        at = pl.ds(pl.multiple_of(b * width, width), width)
        rbias = jnp.broadcast_to(rb[:, at], (SUB, width))
        ibias = jnp.broadcast_to(ib[:, at], (SUB, width))
        rate = jnp.broadcast_to(dr[:, at] * (-8.0 * LOG2E), (SUB, width))
        prod = None
        state = None
        for k in range(seg):
            rows = slice(k * SUB, (k + 1) * SUB)
            rec = 0.5 * jnp.tanh(0.5 * (pre[1, rows, :] + rbias)) + 0.5
            gate = 0.5 * jnp.tanh(0.5 * (pre[2, rows, :] + ibias)) + 0.5
            step = jnp.exp2(rec * rate)
            drive = jnp.sqrt(1.0 - step * step) * (gate * pre[0, rows, :])
            prod = step if k == 0 else prod * step
            state = drive if k == 0 else step * state + drive
            cum[b, rows, :] = prod
            loc[b, rows, :] = state
        cs = jnp.zeros((1, width), F32)
        cp = jnp.ones((1, width), F32)
        for j in range(SUB):
            seg_s[b, j : j + 1, :] = cs
            seg_a[b, j : j + 1, :] = cp
            cs = prod[j : j + 1] * cs + state[j : j + 1]
            cp = prod[j : j + 1] * cp
        lanes = slice(half * width, (half + 1) * width)
        sum_send[g, 0:1, lanes] = cp
        sum_send[g, 1:2, lanes] = cs

    def send_summary(g):
        @pl.loop(me + 1, n)
        def _(to):
            pltpu.make_async_remote_copy(
                src_ref=sum_send.at[g],
                dst_ref=sum_recv.at[me, g],
                send_sem=s_send.at[to],
                recv_sem=s_recv.at[me],
                device_id={"seq": to},
                device_id_type=MESH,
            ).start()

    def summary_slab(other):
        return pltpu.make_async_remote_copy(
            src_ref=sum_send,
            dst_ref=sum_recv.at[other],
            send_sem=s_send.at[other],
            recv_sem=s_recv.at[other],
            device_id={"seq": other},
            device_id_type=MESH,
        )

    mats(0, pre_a)
    pl.semaphore_wait(barrier, n - 1)

    @pl.loop(0, groups - 1)
    def _(g):
        mats(2 * g + 1, pre_b)
        gates(2 * g, g, 0, pre_a)
        mats(2 * g + 2, pre_a)
        gates(2 * g + 1, g, 1, pre_b)
        send_summary(g)

    mats(blocks - 1, pre_b)
    gates(blocks - 2, groups - 1, 0, pre_a)
    gates(blocks - 1, groups - 1, 1, pre_b)
    send_summary(groups - 1)

    def fold(other, state):
        summary_slab(other).wait_recv()
        return tuple(
            sum_recv[other, g, 0:1, :] * state[g] + sum_recv[other, g, 1:2, :]
            for g in range(groups)
        )

    entering = lax.fori_loop(
        0, me, fold, tuple(jnp.zeros((1, 2 * width), F32) for _ in range(groups))
    )
    for g in range(groups):
        carry[2 * g] = entering[g][:, :width]
        carry[2 * g + 1] = entering[g][:, width:]

    @pl.loop(0, blocks)
    def _(b):
        at = pl.ds(pl.multiple_of(b * width, width), width)
        into = seg_s[b] + seg_a[b] * carry[b]
        for k in range(seg // 2):
            rows = slice(2 * k * SUB, (2 * k + 2) * SUB)
            twice = jnp.concatenate([into, into], axis=0)
            hid[rows, at] = (loc[b, rows, :] + cum[b, rows, :] * twice).astype(BF16)

    kvw_copy.wait()
    kvb[me] = dot(hid[...], kvw[...]).astype(BF16)

    def z_copy(s, m, piece):
        rows = pl.ds(piece * piece_rows, piece_rows)
        return pltpu.make_async_remote_copy(
            src_ref=kvb.at[s, rows],
            dst_ref=kvb.at[s, rows],
            send_sem=z_send.at[m, piece],
            recv_sem=kv_recv.at[s, piece],
            device_id={"seq": me + cols},
            device_id_type=MESH,
        )

    def y_copy(s, m, piece, delta):
        rows = pl.ds(piece * piece_rows, piece_rows)
        to = row * cols + lax.rem(col + delta, cols)
        return pltpu.make_async_remote_copy(
            src_ref=kvb.at[s, rows],
            dst_ref=kvb.at[s, rows],
            send_sem=y_send.at[delta - 1, m, piece],
            recv_sem=kv_recv.at[s, piece],
            device_id={"seq": to},
            device_id_type=MESH,
        )

    def arrived(s, piece):
        rows = pl.ds(piece * piece_rows, piece_rows)
        pltpu.make_async_remote_copy(
            src_ref=kvb.at[s, rows],
            dst_ref=kvb.at[s, rows],
            send_sem=z_send.at[0, piece],
            recv_sem=kv_recv.at[s, piece],
            device_id={"seq": lax.rem(me + cols, n)},
            device_id_type=MESH,
        ).wait_recv()

    def goes_up(m):
        return (me + cols < n) & (cols * (m + 1) <= reach + cols - 1)

    def goes_over(s, delta):
        far = row * cols + lax.rem(col + delta, cols) - s
        return (far >= 1) & (far <= reach)

    def forward(s, m, piece):
        @pl.when(goes_up(m))
        def _():
            z_copy(s, m, piece).start()

        for delta in range(1, cols):
            @pl.when(goes_over(s, delta))
            def _():
                y_copy(s, m, piece, delta).start()

    for piece in range(PIECES):
        forward(me, 0, piece)

    factor = scale * LOG2E

    @pl.loop(0, blocks, step=2)
    def _(base):
        for h in (base, base + 1):
            at = pl.ds(pl.multiple_of(h * width, width), width)
            query = dot(unperm[...], hid[:, at]).astype(BF16)
            qn[h] = query
            scores = dot_t(query, kvb[me, :, :head_dim]) + bias[...]
            highest = jnp.max(scores, axis=1, keepdims=True)
            expo = jnp.exp2((scores - highest) * factor)
            top[h] = jnp.broadcast_to(highest, (tok, 128))
            low[h] = functools.reduce(
                jnp.add, [expo[:, c : c + 128] for c in range(0, tok, 128)]
            )
            acc[h] = dot(expo.astype(BF16), kvb[me, :, head_dim:])

    def attend(s, far, masked):
        @pl.loop(0, blocks, step=2)
        def _(base):
            for h in (base, base + 1):
                scores = dot_t(qn[h], kvb[s, :, :head_dim])
                if masked:
                    qrow = lax.broadcasted_iota(jnp.int32, (tok, tok), 0)
                    krow = lax.broadcasted_iota(jnp.int32, (tok, tok), 1)
                    krow = krow // SUB + seg * (krow % SUB)
                    scores = jnp.where(far * tok + qrow - krow < WINDOW, scores, -1e30)
                before = top[h]
                highest = jnp.maximum(before, jnp.max(scores, axis=1, keepdims=True))
                shrink = jnp.exp2((before - highest) * factor)
                parts = [
                    jnp.exp2((scores[:, c : c + 128] - highest) * factor)
                    for c in range(0, tok, 128)
                ]
                top[h] = highest
                low[h] = low[h] * shrink + functools.reduce(jnp.add, parts)
                expo = jnp.concatenate([p.astype(BF16) for p in parts], axis=1)
                update = dot(expo, kvb[s, :, head_dim:])
                for c in range(0, head_dim, 128):
                    acc[h, :, c : c + 128] = (
                        acc[h, :, c : c + 128] * shrink + update[:, c : c + 128]
                    )

    partial = reach * tok + tok - 1 >= WINDOW

    @pl.loop(1, levels + 2)
    def _(m):
        mine = me - cols * m
        held = (m <= levels) & (mine >= 0) & (cols * m <= reach + cols - 1)

        @pl.when(held)
        def _():
            for piece in range(PIECES):
                arrived(mine, piece)
                forward(mine, m, piece)

        @pl.loop(1, cols + 1)
        def _(delta):
            own = delta // cols
            s = row * cols + lax.rem(col + delta, cols) - cols * (m - 1 + own)
            far = me - s
            wanted = (s >= 0) & (far >= 1) & (far <= reach)
            wanted = wanted & (m - 1 + own <= levels)

            @pl.when(wanted & (own == 0))
            def _():
                for piece in range(PIECES):
                    arrived(s, piece)

            if partial:
                @pl.when(wanted & (far * tok + tok - 1 < WINDOW))
                def _():
                    attend(s, far, False)

                @pl.when(wanted & (far * tok + tok - 1 >= WINDOW))
                def _():
                    attend(s, far, True)
            else:
                @pl.when(wanted)
                def _():
                    attend(s, far, False)

    @pl.loop(0, blocks)
    def _(h):
        at = pl.ds(pl.multiple_of(h * width, width), width)
        total = jnp.sum(low[h], axis=1, keepdims=True)
        out[:, at] = (acc[h] * (1.0 / total)).astype(BF16)

    @pl.loop(me + 1, n)
    def _(to):
        summary_slab(to).wait_send()

    @pl.loop(0, levels + 1)
    def _(m):
        s = me - cols * m
        held = (s >= 0) & (cols * m <= reach + cols - 1)
        for piece in range(PIECES):
            @pl.when(held & goes_up(m))
            def _():
                z_copy(s, m, piece).wait_send()

            for delta in range(1, cols):
                @pl.when(held & goes_over(s, delta))
                def _():
                    y_copy(s, m, piece, delta).wait_send()


def on_device(n, inputs, recur_weight, input_weight, recur_bias, input_bias, decay_rate, kv_weight):
    tok, full = inputs.shape
    blocks, width = recur_weight.shape[:2]
    cols = 1
    while 4 * cols * cols <= n:
        cols *= 2
    reach = min((WINDOW + tok - 2) // tok, n - 1)
    levels = min((reach + cols - 1) // cols, n // cols - 1)
    groups = blocks // 2
    head_dim = kv_weight.shape[1] // 2
    vmem = pl.BlockSpec(memory_space=pltpu.VMEM)
    anywhere = pl.BlockSpec(memory_space=pl.ANY)
    dma = pltpu.SemaphoreType.DMA
    return pl.pallas_call(
        functools.partial(fused, n, cols, reach, head_dim ** (-0.5)),
        out_shape=jax.ShapeDtypeStruct((tok, full), BF16),
        in_specs=[anywhere, anywhere, anywhere, vmem, vmem, vmem, anywhere],
        out_specs=vmem,
        scratch_shapes=[
            pltpu.VMEM((blocks, tok, width), BF16),
            pltpu.VMEM((blocks, width, width), BF16),
            pltpu.VMEM((blocks, width, width), BF16),
            pltpu.VMEM(kv_weight.shape, BF16),
            pltpu.VMEM((tok, tok), BF16),
            pltpu.VMEM((tok, tok), BF16),
            pltpu.VMEM((3, tok, width), F32),
            pltpu.VMEM((3, tok, width), F32),
            pltpu.VMEM((blocks, tok, width), F32),
            pltpu.VMEM((blocks, tok, width), F32),
            pltpu.VMEM((blocks, SUB, width), F32),
            pltpu.VMEM((blocks, SUB, width), F32),
            pltpu.VMEM((groups, 2, 2 * width), F32),
            pltpu.VMEM((n, groups, 2, 2 * width), F32),
            pltpu.VMEM((blocks, 1, width), F32),
            pltpu.VMEM((tok, full), BF16),
            pltpu.VMEM((blocks, tok, width), BF16),
            pltpu.VMEM((n, tok, 2 * head_dim), BF16),
            pltpu.VMEM((blocks, tok, 128), F32),
            pltpu.VMEM((blocks, tok, 128), F32),
            pltpu.VMEM((blocks, tok, width), F32),
            pltpu.VMEM((tok, tok), F32),
            dma((3, blocks)),
            dma,
            dma((n,)),
            dma((n,)),
            dma((levels + 1, PIECES)),
            dma((max(cols - 1, 1), levels + 1, PIECES)),
            dma((n, PIECES)),
        ],
        compiler_params=pltpu.CompilerParams(
            collective_id=0, has_side_effects=True, vmem_limit_bytes=60 * 1024 * 1024
        ),
    )(
        inputs,
        recur_weight,
        input_weight,
        recur_bias.reshape(1, full),
        input_bias.reshape(1, full),
        decay_rate.reshape(1, full),
        kv_weight,
    )


def solution(mesh):
    placed = (P(("batch", "seq"), None), P(), P(), P(), P(), P(), P())
    return jax.shard_map(
        functools.partial(on_device, mesh.shape["seq"]),
        mesh=mesh,
        in_specs=placed,
        out_specs=P(("batch", "seq"), None),
        check_vma=False,
    )
```

```python
import functools
import math

import jax
import jax.numpy as jnp
from jax import lax
from jax.experimental import pallas as pl
from jax.experimental.pallas import tpu as pltpu
from jax.sharding import PartitionSpec as P

WINDOW = 2048
SUB = 8
PIECES = 2
HEADS = 4
EXTRA = 16
MESH = pl.DeviceIdType.MESH
LOG2E = math.log2(math.e)
F32 = jnp.float32
BF16 = jnp.bfloat16


def dot(a, b):
    return jnp.dot(a, b, preferred_element_type=F32)


def dot_t(a, b):
    return lax.dot_general(a, b, (((1,), (1,)), ((), ())), preferred_element_type=F32)


def fused(
    n, cols, reach, scale,
    x_hbm, rw_hbm, iw_hbm, rb, ib, dr, kvw_hbm,
    out,
    xv, rwv, iwv, kvw, perm, unperm, pre_a, pre_b, cum, loc, seg_a, seg_s, sum_send, sum_recv,
    carry, hid, qt, kb, vt, top, acc, bias,
    in_sem, kvw_sem, s_send, s_recv, z_send, y_send, kv_recv,
):
    me = lax.axis_index("seq")
    row = me // cols
    col = me % cols
    blocks, tok, width = xv.shape
    seg = tok // SUB
    groups = blocks // 2
    head_dim = width
    extra = vt.shape[1] - head_dim
    levels = z_send.shape[0] - 1

    def in_copies(b):
        at = pl.ds(pl.multiple_of(b * width, width), width)
        return (
            pltpu.make_async_copy(x_hbm.at[:, at], xv.at[b], in_sem.at[0, b]),
            pltpu.make_async_copy(rw_hbm.at[b], rwv.at[b], in_sem.at[1, b]),
            pltpu.make_async_copy(iw_hbm.at[b], iwv.at[b], in_sem.at[2, b]),
        )

    @pl.loop(0, blocks)
    def _(b):
        for copy in in_copies(b):
            copy.start()

    kvw_copy = pltpu.make_async_copy(kvw_hbm, kvw, kvw_sem)
    kvw_copy.start()

    barrier = pltpu.get_barrier_semaphore()

    @pl.loop(1, n)
    def _(d):
        pl.semaphore_signal(
            barrier, inc=1, device_id={"seq": lax.rem(me + d, n)}, device_id_type=MESH
        )

    first = lax.broadcasted_iota(jnp.int32, (tok, tok), 0)
    second = lax.broadcasted_iota(jnp.int32, (tok, tok), 1)
    place_1 = second // SUB + seg * (second % SUB)
    place_0 = first // SUB + seg * (first % SUB)
    perm[...] = jnp.where(second == place_0, 1.0, 0.0).astype(BF16)
    unperm[...] = jnp.where(first == place_1, 1.0, 0.0).astype(BF16)
    bias[...] = jnp.where(place_0 <= place_1, 0.0, -1e30)
    ones = jnp.where(lax.broadcasted_iota(jnp.int32, (extra, tok), 0) == 0, 1.0, 0.0)

    @pl.loop(0, n)
    def _(s):
        vt[s, head_dim:] = ones.astype(BF16)


    def mats(b, pre):
        for copy in in_copies(b):
            copy.wait()
        moved = dot(perm[...], xv[b])
        moved = moved * 0.5
        small = moved.astype(BF16)
        pre[0] = moved
        pre[1] = dot(small, rwv[b])
        pre[2] = dot(small, iwv[b])

    def gates(b, g, half, pre):
        at = pl.ds(pl.multiple_of(b * width, width), width)
        rbias = jnp.broadcast_to(rb[:, at] * 0.5, (SUB, width))
        ibias = jnp.broadcast_to(ib[:, at] * 0.5, (SUB, width))
        rate = jnp.broadcast_to(dr[:, at] * (-4.0 * LOG2E), (SUB, width))
        prod = None
        state = None
        for k in range(seg):
            rows = slice(k * SUB, (k + 1) * SUB)
            rec = jnp.tanh(pre[1, rows, :] + rbias)
            gate = jnp.tanh(pre[2, rows, :] + ibias) + 1.0
            step = jnp.exp2(rec * rate + rate)
            rest = jnp.maximum(1.0 - step * step, 1e-36)
            drive = (rest * lax.rsqrt(rest)) * (gate * pre[0, rows, :])
            prod = step if k == 0 else prod * step
            state = drive if k == 0 else step * state + drive
            cum[b, rows, :] = prod
            loc[b, rows, :] = state
        cs = jnp.zeros((1, width), F32)
        cp = jnp.ones((1, width), F32)
        for j in range(SUB):
            seg_s[b, j : j + 1, :] = cs
            seg_a[b, j : j + 1, :] = cp
            cs = prod[j : j + 1] * cs + state[j : j + 1]
            cp = prod[j : j + 1] * cp
        lanes = slice(half * width, (half + 1) * width)
        sum_send[g, 0:1, lanes] = cp
        sum_send[g, 1:2, lanes] = cs

    def send_summary(g):
        @pl.loop(me + 1, n)
        def _(to):
            pltpu.make_async_remote_copy(
                src_ref=sum_send.at[g],
                dst_ref=sum_recv.at[me, g],
                send_sem=s_send.at[to],
                recv_sem=s_recv.at[me],
                device_id={"seq": to},
                device_id_type=MESH,
            ).start()

    def summary_slab(other):
        return pltpu.make_async_remote_copy(
            src_ref=sum_send,
            dst_ref=sum_recv.at[other],
            send_sem=s_send.at[other],
            recv_sem=s_recv.at[other],
            device_id={"seq": other},
            device_id_type=MESH,
        )

    mats(0, pre_a)
    pl.semaphore_wait(barrier, n - 1)

    @pl.loop(0, groups - 1)
    def _(g):
        mats(2 * g + 1, pre_b)
        gates(2 * g, g, 0, pre_a)
        mats(2 * g + 2, pre_a)
        gates(2 * g + 1, g, 1, pre_b)
        send_summary(g)

    mats(blocks - 1, pre_b)
    gates(blocks - 2, groups - 1, 0, pre_a)
    gates(blocks - 1, groups - 1, 1, pre_b)
    send_summary(groups - 1)

    def fold(other, state):
        summary_slab(other).wait_recv()
        return tuple(
            sum_recv[other, g, 0:1, :] * state[g] + sum_recv[other, g, 1:2, :]
            for g in range(groups)
        )

    entering = lax.fori_loop(
        0, me, fold, tuple(jnp.zeros((1, 2 * width), F32) for _ in range(groups))
    )
    for g in range(groups):
        carry[2 * g] = entering[g][:, :width]
        carry[2 * g + 1] = entering[g][:, width:]

    @pl.loop(0, blocks)
    def _(b):
        at = pl.ds(pl.multiple_of(b * width, width), width)
        into = seg_s[b] + seg_a[b] * carry[b]
        for k in range(seg // 2):
            rows = slice(2 * k * SUB, (2 * k + 2) * SUB)
            twice = jnp.concatenate([into, into], axis=0)
            hid[rows, at] = (loc[b, rows, :] + cum[b, rows, :] * twice).astype(BF16)

    def piece_of(s, piece):
        return kb.at[s] if piece == 0 else vt.at[s, pl.ds(0, head_dim)]

    def z_copy(s, m, piece):
        part = piece_of(s, piece)
        return pltpu.make_async_remote_copy(
            src_ref=part,
            dst_ref=part,
            send_sem=z_send.at[m, piece],
            recv_sem=kv_recv.at[s, piece],
            device_id={"seq": me + cols},
            device_id_type=MESH,
        )

    def y_copy(s, m, piece, delta):
        part = piece_of(s, piece)
        to = row * cols + lax.rem(col + delta, cols)
        return pltpu.make_async_remote_copy(
            src_ref=part,
            dst_ref=part,
            send_sem=y_send.at[delta - 1, m, piece],
            recv_sem=kv_recv.at[s, piece],
            device_id={"seq": to},
            device_id_type=MESH,
        )

    def arrived(s, piece):
        part = piece_of(s, piece)
        pltpu.make_async_remote_copy(
            src_ref=part,
            dst_ref=part,
            send_sem=z_send.at[0, piece],
            recv_sem=kv_recv.at[s, piece],
            device_id={"seq": lax.rem(me + cols, n)},
            device_id_type=MESH,
        ).wait_recv()

    def goes_up(m):
        return (me + cols < n) & (cols * (m + 1) <= reach + cols - 1)

    def goes_over(s, delta):
        far = row * cols + lax.rem(col + delta, cols) - s
        return (far >= 1) & (far <= reach)

    def forward(s, m, piece):
        @pl.when(goes_up(m))
        def _():
            z_copy(s, m, piece).start()

        for delta in range(1, cols):
            @pl.when(goes_over(s, delta))
            def _():
                y_copy(s, m, piece, delta).start()

    kvw_copy.wait()
    kb[me] = dot(hid[...], kvw[:, :head_dim]).astype(BF16)
    forward(me, 0, 0)
    vt[me, :head_dim] = dot(hid[...], kvw[:, head_dim:]).T.astype(BF16)
    forward(me, 0, 1)

    factor = scale * LOG2E

    @pl.loop(0, blocks, step=HEADS)
    def _(base):
        for h in [base + i for i in range(HEADS)]:
            at = pl.ds(pl.multiple_of(h * width, width), width)
            query = hid[:, at].astype(F32).T.astype(BF16)
            qt[h] = query
            scores = dot(kb[me], query) + bias[...]
            highest = jnp.max(scores, axis=0, keepdims=True)
            top[h] = highest
            expo = jnp.exp2((scores - highest) * factor).astype(BF16)
            acc[h] = dot(vt[me], expo)

    def attend(s, far, masked):
        @pl.loop(0, blocks, step=HEADS)
        def _(base):
            for h in [base + i for i in range(HEADS)]:
                scores = dot(kb[s], qt[h])
                if masked:
                    krow = lax.broadcasted_iota(jnp.int32, (tok, tok), 0)
                    krow = krow // SUB + seg * (krow % SUB)
                    qrow = lax.broadcasted_iota(jnp.int32, (tok, tok), 1)
                    qrow = qrow // SUB + seg * (qrow % SUB)
                    scores = jnp.where(far * tok + qrow - krow < WINDOW, scores, -1e30)
                before = top[h]
                highest = jnp.maximum(before, jnp.max(scores, axis=0, keepdims=True))
                shrink = jnp.exp2((before - highest) * factor)
                top[h] = highest
                expo = jnp.exp2((scores - highest) * factor).astype(BF16)
                acc[h] = acc[h] * shrink + dot(vt[s], expo)

    partial = reach * tok + tok - 1 >= WINDOW

    @pl.loop(1, levels + 2)
    def _(m):
        mine = me - cols * m
        held = (m <= levels) & (mine >= 0) & (cols * m <= reach + cols - 1)

        @pl.when(held)
        def _():
            for piece in range(PIECES):
                arrived(mine, piece)
                forward(mine, m, piece)

        @pl.loop(1, cols + 1)
        def _(delta):
            own = delta // cols
            s = row * cols + lax.rem(col + delta, cols) - cols * (m - 1 + own)
            far = me - s
            wanted = (s >= 0) & (far >= 1) & (far <= reach)
            wanted = wanted & (m - 1 + own <= levels)

            @pl.when(wanted & (own == 0))
            def _():
                for piece in range(PIECES):
                    arrived(s, piece)

            if partial:
                @pl.when(wanted & (far * tok + tok - 1 < WINDOW))
                def _():
                    attend(s, far, False)

                @pl.when(wanted & (far * tok + tok - 1 >= WINDOW))
                def _():
                    attend(s, far, True)
            else:
                @pl.when(wanted)
                def _():
                    attend(s, far, False)

    @pl.loop(0, blocks)
    def _(h):
        at = pl.ds(pl.multiple_of(h * width, width), width)
        mean = acc[h, :head_dim] * (1.0 / acc[h, head_dim : head_dim + 1])
        out[:, at] = dot_t(unperm[...], mean.astype(BF16)).astype(BF16)

    @pl.loop(me + 1, n)
    def _(to):
        summary_slab(to).wait_send()

    @pl.loop(0, levels + 1)
    def _(m):
        s = me - cols * m
        held = (s >= 0) & (cols * m <= reach + cols - 1)
        for piece in range(PIECES):
            @pl.when(held & goes_up(m))
            def _():
                z_copy(s, m, piece).wait_send()

            for delta in range(1, cols):
                @pl.when(held & goes_over(s, delta))
                def _():
                    y_copy(s, m, piece, delta).wait_send()


def on_device(n, inputs, recur_weight, input_weight, recur_bias, input_bias, decay_rate, kv_weight):
    tok, full = inputs.shape
    blocks, width = recur_weight.shape[:2]
    cols = 1
    while 4 * cols * cols <= n:
        cols *= 2
    reach = min((WINDOW + tok - 2) // tok, n - 1)
    levels = min((reach + cols - 1) // cols, n // cols - 1)
    groups = blocks // 2
    head_dim = kv_weight.shape[1] // 2
    vmem = pl.BlockSpec(memory_space=pltpu.VMEM)
    anywhere = pl.BlockSpec(memory_space=pl.ANY)
    dma = pltpu.SemaphoreType.DMA
    return pl.pallas_call(
        functools.partial(fused, n, cols, reach, head_dim ** (-0.5)),
        out_shape=jax.ShapeDtypeStruct((tok, full), BF16),
        in_specs=[anywhere, anywhere, anywhere, vmem, vmem, vmem, anywhere],
        out_specs=vmem,
        scratch_shapes=[
            pltpu.VMEM((blocks, tok, width), BF16),
            pltpu.VMEM((blocks, width, width), BF16),
            pltpu.VMEM((blocks, width, width), BF16),
            pltpu.VMEM(kv_weight.shape, BF16),
            pltpu.VMEM((tok, tok), BF16),
            pltpu.VMEM((tok, tok), BF16),
            pltpu.VMEM((3, tok, width), F32),
            pltpu.VMEM((3, tok, width), F32),
            pltpu.VMEM((blocks, tok, width), F32),
            pltpu.VMEM((blocks, tok, width), F32),
            pltpu.VMEM((blocks, SUB, width), F32),
            pltpu.VMEM((blocks, SUB, width), F32),
            pltpu.VMEM((groups, 2, 2 * width), F32),
            pltpu.VMEM((n, groups, 2, 2 * width), F32),
            pltpu.VMEM((blocks, 1, width), F32),
            pltpu.VMEM((tok, full), BF16),
            pltpu.VMEM((blocks, head_dim, tok), BF16),
            pltpu.VMEM((n, tok, head_dim), BF16),
            pltpu.VMEM((n, head_dim + EXTRA, tok), BF16),
            pltpu.VMEM((blocks, 1, tok), F32),
            pltpu.VMEM((blocks, head_dim + EXTRA, tok), F32),
            pltpu.VMEM((tok, tok), F32),
            dma((3, blocks)),
            dma,
            dma((n,)),
            dma((n,)),
            dma((levels + 1, PIECES)),
            dma((max(cols - 1, 1), levels + 1, PIECES)),
            dma((n, PIECES)),
        ],
        compiler_params=pltpu.CompilerParams(
            collective_id=0, has_side_effects=True, vmem_limit_bytes=60 * 1024 * 1024
        ),
    )(
        inputs,
        recur_weight,
        input_weight,
        recur_bias.reshape(1, full),
        input_bias.reshape(1, full),
        decay_rate.reshape(1, full),
        kv_weight,
    )


def solution(mesh):
    placed = (P(("batch", "seq"), None), P(), P(), P(), P(), P(), P())
    return jax.shard_map(
        functools.partial(on_device, mesh.shape["seq"]),
        mesh=mesh,
        in_specs=placed,
        out_specs=P(("batch", "seq"), None),
        check_vma=False,
    )
```

```python
import functools
import math

import jax
import jax.numpy as jnp
from jax import lax
from jax.experimental import pallas as pl
from jax.experimental.pallas import tpu as pltpu
from jax.sharding import PartitionSpec as P

WINDOW = 2048
SUB = 8
PIECES = 2
HEADS = 16
EXTRA = 16
MESH = pl.DeviceIdType.MESH
LOG2E = math.log2(math.e)
F32 = jnp.float32
BF16 = jnp.bfloat16


def dot(a, b):
    return jnp.dot(a, b, preferred_element_type=F32)


def dot_t(a, b):
    return lax.dot_general(a, b, (((1,), (1,)), ((), ())), preferred_element_type=F32)


def fused(
    n, cols, reach, scale,
    x_hbm, rw_hbm, iw_hbm, rb, ib, dr, kvw_hbm,
    out,
    xv, rwv, iwv, kvw, perm, unperm, pre_a, pre_b, cum, loc, seg_a, seg_s, sum_send, sum_recv,
    carry, hid, qt, kb, vt, top, acc, bias,
    in_sem, kvw_sem, s_send, s_recv, z_send, y_send, kv_recv,
):
    me = lax.axis_index("seq")
    row = me // cols
    col = me % cols
    blocks, tok, width = xv.shape
    seg = tok // SUB
    groups = blocks // 2
    head_dim = width
    extra = vt.shape[1] - head_dim
    levels = z_send.shape[0] - 1

    def in_copies(b):
        at = pl.ds(pl.multiple_of(b * width, width), width)
        return (
            pltpu.make_async_copy(x_hbm.at[:, at], xv.at[b], in_sem.at[0, b]),
            pltpu.make_async_copy(rw_hbm.at[b], rwv.at[b], in_sem.at[1, b]),
            pltpu.make_async_copy(iw_hbm.at[b], iwv.at[b], in_sem.at[2, b]),
        )

    @pl.loop(0, blocks)
    def _(b):
        for copy in in_copies(b):
            copy.start()

    kvw_copy = pltpu.make_async_copy(kvw_hbm, kvw, kvw_sem)
    kvw_copy.start()

    barrier = pltpu.get_barrier_semaphore()

    @pl.loop(1, n)
    def _(d):
        pl.semaphore_signal(
            barrier, inc=1, device_id={"seq": lax.rem(me + d, n)}, device_id_type=MESH
        )

    first = lax.broadcasted_iota(jnp.int32, (tok, tok), 0)
    second = lax.broadcasted_iota(jnp.int32, (tok, tok), 1)
    place_1 = second // SUB + seg * (second % SUB)
    place_0 = first // SUB + seg * (first % SUB)
    perm[...] = jnp.where(second == place_0, 1.0, 0.0).astype(BF16)
    unperm[...] = jnp.where(first == place_1, 1.0, 0.0).astype(BF16)
    bias[...] = jnp.where(place_0 <= place_1, 0.0, -1e30)
    ones = jnp.where(lax.broadcasted_iota(jnp.int32, (extra, tok), 0) == 0, 1.0, 0.0)

    @pl.loop(0, n)
    def _(s):
        vt[s, head_dim:] = ones.astype(BF16)


    def mats(b, pre):
        for copy in in_copies(b):
            copy.wait()
        moved = dot(perm[...], xv[b])
        moved = moved * 0.5
        small = moved.astype(BF16)
        pre[0] = moved
        pre[1] = dot(small, rwv[b])
        pre[2] = dot(small, iwv[b])

    def gates(b, g, half, pre):
        at = pl.ds(pl.multiple_of(b * width, width), width)
        rbias = jnp.broadcast_to(rb[:, at] * 0.5, (SUB, width))
        ibias = jnp.broadcast_to(ib[:, at] * 0.5, (SUB, width))
        rate = jnp.broadcast_to(dr[:, at] * (-4.0 * LOG2E), (SUB, width))
        prod = None
        state = None
        for k in range(seg):
            rows = slice(k * SUB, (k + 1) * SUB)
            rec = jnp.tanh(pre[1, rows, :] + rbias)
            gate = jnp.tanh(pre[2, rows, :] + ibias) + 1.0
            step = jnp.exp2(rec * rate + rate)
            rest = jnp.maximum(1.0 - step * step, 1e-36)
            drive = (rest * lax.rsqrt(rest)) * (gate * pre[0, rows, :])
            prod = step if k == 0 else prod * step
            state = drive if k == 0 else step * state + drive
            cum[b, rows, :] = prod
            loc[b, rows, :] = state
        cs = jnp.zeros((1, width), F32)
        cp = jnp.ones((1, width), F32)
        for j in range(SUB):
            seg_s[b, j : j + 1, :] = cs
            seg_a[b, j : j + 1, :] = cp
            cs = prod[j : j + 1] * cs + state[j : j + 1]
            cp = prod[j : j + 1] * cp
        lanes = slice(half * width, (half + 1) * width)
        sum_send[g, 0:1, lanes] = cp
        sum_send[g, 1:2, lanes] = cs

    def send_summary(g):
        @pl.loop(me + 1, n)
        def _(to):
            pltpu.make_async_remote_copy(
                src_ref=sum_send.at[g],
                dst_ref=sum_recv.at[me, g],
                send_sem=s_send.at[to],
                recv_sem=s_recv.at[me],
                device_id={"seq": to},
                device_id_type=MESH,
            ).start()

    def summary_slab(other):
        return pltpu.make_async_remote_copy(
            src_ref=sum_send,
            dst_ref=sum_recv.at[other],
            send_sem=s_send.at[other],
            recv_sem=s_recv.at[other],
            device_id={"seq": other},
            device_id_type=MESH,
        )

    mats(0, pre_a)
    pl.semaphore_wait(barrier, n - 1)

    @pl.loop(0, groups - 1)
    def _(g):
        mats(2 * g + 1, pre_b)
        gates(2 * g, g, 0, pre_a)
        mats(2 * g + 2, pre_a)
        gates(2 * g + 1, g, 1, pre_b)
        send_summary(g)

    mats(blocks - 1, pre_b)
    gates(blocks - 2, groups - 1, 0, pre_a)
    gates(blocks - 1, groups - 1, 1, pre_b)
    send_summary(groups - 1)

    def fold(other, state):
        summary_slab(other).wait_recv()
        return tuple(
            sum_recv[other, g, 0:1, :] * state[g] + sum_recv[other, g, 1:2, :]
            for g in range(groups)
        )

    entering = lax.fori_loop(
        0, me, fold, tuple(jnp.zeros((1, 2 * width), F32) for _ in range(groups))
    )
    for g in range(groups):
        carry[2 * g] = entering[g][:, :width]
        carry[2 * g + 1] = entering[g][:, width:]

    @pl.loop(0, blocks, step=2)
    def _(base):
        for b in (base, base + 1):
            at = pl.ds(pl.multiple_of(b * width, width), width)
            into = seg_s[b] + seg_a[b] * carry[b]
            twice = jnp.concatenate([into, into], axis=0)
            for k in range(seg // 2):
                rows = slice(2 * k * SUB, (2 * k + 2) * SUB)
                hid[rows, at] = (loc[b, rows, :] + cum[b, rows, :] * twice).astype(BF16)

    def piece_of(s, piece):
        return kb.at[s] if piece == 0 else vt.at[s, pl.ds(0, head_dim)]

    def z_copy(s, m, piece):
        part = piece_of(s, piece)
        return pltpu.make_async_remote_copy(
            src_ref=part,
            dst_ref=part,
            send_sem=z_send.at[m, piece],
            recv_sem=kv_recv.at[s, piece],
            device_id={"seq": me + cols},
            device_id_type=MESH,
        )

    def y_copy(s, m, piece, delta):
        part = piece_of(s, piece)
        to = row * cols + lax.rem(col + delta, cols)
        return pltpu.make_async_remote_copy(
            src_ref=part,
            dst_ref=part,
            send_sem=y_send.at[delta - 1, m, piece],
            recv_sem=kv_recv.at[s, piece],
            device_id={"seq": to},
            device_id_type=MESH,
        )

    def arrived(s, piece):
        part = piece_of(s, piece)
        pltpu.make_async_remote_copy(
            src_ref=part,
            dst_ref=part,
            send_sem=z_send.at[0, piece],
            recv_sem=kv_recv.at[s, piece],
            device_id={"seq": lax.rem(me + cols, n)},
            device_id_type=MESH,
        ).wait_recv()

    def goes_up(m):
        return (me + cols < n) & (cols * (m + 1) <= reach + cols - 1)

    def goes_over(s, delta):
        far = row * cols + lax.rem(col + delta, cols) - s
        return (far >= 1) & (far <= reach)

    def forward(s, m, piece):
        @pl.when(goes_up(m))
        def _():
            z_copy(s, m, piece).start()

        for delta in range(1, cols):
            @pl.when(goes_over(s, delta))
            def _():
                y_copy(s, m, piece, delta).start()

    kvw_copy.wait()
    kb[me] = dot(hid[...], kvw[:, :head_dim]).astype(BF16)
    forward(me, 0, 0)
    vt[me, :head_dim] = dot(hid[...], kvw[:, head_dim:]).T.astype(BF16)
    forward(me, 0, 1)

    factor = scale * LOG2E

    @pl.loop(0, blocks, step=HEADS)
    def _(base):
        for h in [base + i for i in range(HEADS)]:
            at = pl.ds(pl.multiple_of(h * width, width), width)
            query = hid[:, at].astype(F32).T.astype(BF16)
            qt[h] = query
            scores = dot(kb[me], query) + bias[...]
            highest = jnp.max(scores, axis=0, keepdims=True)
            top[h] = highest
            expo = jnp.exp2((scores - highest) * factor).astype(BF16)
            acc[h] = dot(vt[me], expo)

    def attend(s, far, masked):
        @pl.loop(0, blocks, step=HEADS)
        def _(base):
            for h in [base + i for i in range(HEADS)]:
                scores = dot(kb[s], qt[h])
                if masked:
                    krow = lax.broadcasted_iota(jnp.int32, (tok, tok), 0)
                    krow = krow // SUB + seg * (krow % SUB)
                    qrow = lax.broadcasted_iota(jnp.int32, (tok, tok), 1)
                    qrow = qrow // SUB + seg * (qrow % SUB)
                    scores = jnp.where(far * tok + qrow - krow < WINDOW, scores, -1e30)
                before = top[h]
                highest = jnp.maximum(before, jnp.max(scores, axis=0, keepdims=True))
                shrink = jnp.exp2((before - highest) * factor)
                top[h] = highest
                expo = jnp.exp2((scores - highest) * factor).astype(BF16)
                acc[h] = acc[h] * shrink + dot(vt[s], expo)

    partial = reach * tok + tok - 1 >= WINDOW

    @pl.loop(1, levels + 2)
    def _(m):
        mine = me - cols * m
        held = (m <= levels) & (mine >= 0) & (cols * m <= reach + cols - 1)

        @pl.when(held)
        def _():
            for piece in range(PIECES):
                arrived(mine, piece)
                forward(mine, m, piece)

        @pl.loop(1, cols + 1)
        def _(delta):
            own = delta // cols
            s = row * cols + lax.rem(col + delta, cols) - cols * (m - 1 + own)
            far = me - s
            wanted = (s >= 0) & (far >= 1) & (far <= reach)
            wanted = wanted & (m - 1 + own <= levels)

            @pl.when(wanted & (own == 0))
            def _():
                for piece in range(PIECES):
                    arrived(s, piece)

            if partial:
                @pl.when(wanted & (far * tok + tok - 1 < WINDOW))
                def _():
                    attend(s, far, False)

                @pl.when(wanted & (far * tok + tok - 1 >= WINDOW))
                def _():
                    attend(s, far, True)
            else:
                @pl.when(wanted)
                def _():
                    attend(s, far, False)

    @pl.loop(0, blocks, step=HEADS)
    def _(base):
        for h in [base + i for i in range(HEADS)]:
            at = pl.ds(pl.multiple_of(h * width, width), width)
            mean = acc[h, :head_dim] * (1.0 / acc[h, head_dim : head_dim + 1])
            out[:, at] = dot_t(unperm[...], mean.astype(BF16)).astype(BF16)

    @pl.loop(me + 1, n)
    def _(to):
        summary_slab(to).wait_send()

    @pl.loop(0, levels + 1)
    def _(m):
        s = me - cols * m
        held = (s >= 0) & (cols * m <= reach + cols - 1)
        for piece in range(PIECES):
            @pl.when(held & goes_up(m))
            def _():
                z_copy(s, m, piece).wait_send()

            for delta in range(1, cols):
                @pl.when(held & goes_over(s, delta))
                def _():
                    y_copy(s, m, piece, delta).wait_send()


def on_device(n, inputs, recur_weight, input_weight, recur_bias, input_bias, decay_rate, kv_weight):
    tok, full = inputs.shape
    blocks, width = recur_weight.shape[:2]
    cols = 1
    while 4 * cols * cols <= n:
        cols *= 2
    reach = min((WINDOW + tok - 2) // tok, n - 1)
    levels = min((reach + cols - 1) // cols, n // cols - 1)
    groups = blocks // 2
    head_dim = kv_weight.shape[1] // 2
    vmem = pl.BlockSpec(memory_space=pltpu.VMEM)
    anywhere = pl.BlockSpec(memory_space=pl.ANY)
    dma = pltpu.SemaphoreType.DMA
    return pl.pallas_call(
        functools.partial(fused, n, cols, reach, head_dim ** (-0.5)),
        out_shape=jax.ShapeDtypeStruct((tok, full), BF16),
        in_specs=[anywhere, anywhere, anywhere, vmem, vmem, vmem, anywhere],
        out_specs=vmem,
        scratch_shapes=[
            pltpu.VMEM((blocks, tok, width), BF16),
            pltpu.VMEM((blocks, width, width), BF16),
            pltpu.VMEM((blocks, width, width), BF16),
            pltpu.VMEM(kv_weight.shape, BF16),
            pltpu.VMEM((tok, tok), BF16),
            pltpu.VMEM((tok, tok), BF16),
            pltpu.VMEM((3, tok, width), F32),
            pltpu.VMEM((3, tok, width), F32),
            pltpu.VMEM((blocks, tok, width), F32),
            pltpu.VMEM((blocks, tok, width), F32),
            pltpu.VMEM((blocks, SUB, width), F32),
            pltpu.VMEM((blocks, SUB, width), F32),
            pltpu.VMEM((groups, 2, 2 * width), F32),
            pltpu.VMEM((n, groups, 2, 2 * width), F32),
            pltpu.VMEM((blocks, 1, width), F32),
            pltpu.VMEM((tok, full), BF16),
            pltpu.VMEM((blocks, head_dim, tok), BF16),
            pltpu.VMEM((n, tok, head_dim), BF16),
            pltpu.VMEM((n, head_dim + EXTRA, tok), BF16),
            pltpu.VMEM((blocks, 1, tok), F32),
            pltpu.VMEM((blocks, head_dim + EXTRA, tok), F32),
            pltpu.VMEM((tok, tok), F32),
            dma((3, blocks)),
            dma,
            dma((n,)),
            dma((n,)),
            dma((levels + 1, PIECES)),
            dma((max(cols - 1, 1), levels + 1, PIECES)),
            dma((n, PIECES)),
        ],
        compiler_params=pltpu.CompilerParams(
            collective_id=0, has_side_effects=True, vmem_limit_bytes=60 * 1024 * 1024
        ),
    )(
        inputs,
        recur_weight,
        input_weight,
        recur_bias.reshape(1, full),
        input_bias.reshape(1, full),
        decay_rate.reshape(1, full),
        kv_weight,
    )


def solution(mesh):
    placed = (P(("batch", "seq"), None), P(), P(), P(), P(), P(), P())
    return jax.shard_map(
        functools.partial(on_device, mesh.shape["seq"]),
        mesh=mesh,
        in_specs=placed,
        out_specs=P(("batch", "seq"), None),
        check_vma=False,
    )
```
